256 devices in a mesh: groups: 2 (over z), row: 128 (over x, y, core).
Axes of the slice: x: 8, y: 8, z: 2, core: 2. Of those that a mesh axis runs over, the one named last changes fastest.
The devices are a block of a 8x8x16 slice.
Arguments:
- matrix_a: float32 [49152, 1024], P(('groups', 'row')), parts along dimension 0, may hold values from -0.76546554 to 0.76546554, as said below
- matrix_b: float32 [49152, 1024], P(('groups', 'row')), parts along dimension 0, may hold values from -6 to 6
Outputs:
- first_factor: float32 [2048, 1024], P(('groups', 'row')), parts along dimension 0
- factor: float32 [2048, 1024], P(('groups', 'row')), parts along dimension 0
- projection: float32 [2048, 1024], P(('groups', 'row')), parts along dimension 0
The draws below stay inside these ranges and needn't reach their ends.
There are 2 independent parts, one for each index of `groups`. The reference program is written for one: setup_inputs(seed, part) draws one part's arguments, and reference() takes and returns one part's arrays. A program takes and returns all parts, laid end to end along the dimension named above; each array names one. Nothing has to cross between parts.
Inputs may be any that keep to these rules, and one draw needn't show every extreme that they name: `matrix_a`: A real matrix of full column rank.
All inputs are finite; a program needn't handle non-finite values.
Results may differ from the reference program's by a relative error of at most 0.0003.
Values sent between devices are 32-bit elements; how exact they have to be, the bound alone decides.
No kernel may reach another device: no remote copies, remote signals or barrier semaphores. Data moves between devices by JAX's collectives and lax.ppermute only.
A program may use at most 128 MiB of HBM per device.

```python
import math
import jax
import jax.numpy as jnp
from jax import lax

N = 1024
ROWS = 24576


def draw_matrix_a(key, part):
    keys = jax.random.split(jax.random.fold_in(key, 7), 5)
    position = jnp.arange(ROWS, dtype=jnp.float32) / ROWS
    jitter = jax.random.uniform(keys[1], (ROWS,), jnp.float32, -0.05, 0.05)
    top = 4.0
    spread = 0.25
    level = 0.05
    noise = jnp.clip(jax.random.normal(keys[0], (ROWS, N), jnp.float32), -6.0, 6.0)
    column_scale = 10.0 ** jax.random.uniform(keys[2], (N,), jnp.float32, -spread, spread)
    components = min(128, N // 2)
    weights = 0.9 ** jnp.arange(components, dtype=jnp.float32)
    weight_norm = jnp.sqrt(jnp.sum(weights * weights))
    left = jax.random.uniform(keys[3], (ROWS, components), jnp.float32, -1.732, 1.732)
    right = jax.random.uniform(keys[4], (components, N), jnp.float32, -1.732, 1.732)
    shared = jnp.dot(left * weights[None, :], right, precision=lax.Precision.HIGHEST, preferred_element_type=jnp.float32) / weight_norm
    row_scale = top ** (position + jitter)
    mean_square = (top * top - 1.0) / (2.0 * math.log(top))
    shared = shared * (row_scale[:, None] / math.sqrt(mean_square))
    return (shared + level * noise) * column_scale[None, :] / math.sqrt(ROWS)


def block_levels(own_key, shape, cuts, low, top_value):
    gain = 1.0
    for dim, blocks in cuts:
        steps = jax.random.uniform(jax.random.fold_in(jax.random.fold_in(own_key, 6), dim), (blocks,), jnp.float32, low / len(cuts), top_value / len(cuts))
        gain = gain * jnp.repeat(jnp.exp(steps), shape[dim] // blocks).reshape((-1,) + (1,) * (len(shape) - 1 - dim))
    return gain


def normal_values(own_key, extent, scale, limit, cuts=(), kind=jnp.bfloat16):
    factor_of = block_levels(own_key, extent, cuts, -0.22, 0.18) if cuts else 1.0
    values = jax.random.normal(own_key, extent, jnp.float32) * scale * factor_of
    return jnp.minimum(jnp.maximum(values, -limit), limit).astype(kind)


def setup_inputs(seed: int = 0, part: int = 0) -> dict:
    splits = jax.random.split(jax.random.key(seed), 3)
    part_keys = jax.random.split(jax.random.fold_in(splits[2], part), 3)
    return {
        "matrix_a": draw_matrix_a(jax.random.fold_in(jax.random.fold_in(splits[2], part), 71), part),
        "matrix_b": normal_values(part_keys[1], (ROWS, N), 1.0, 6.0, ((0, 128),), jnp.float32),
    }


def reference(matrix_a, matrix_b):
    highest = lax.Precision.HIGHEST
    gram1 = jnp.dot(matrix_a.T.astype(jnp.float32), matrix_a.astype(jnp.float32), precision=highest, preferred_element_type=jnp.float32)
    shift = jnp.trace(gram1) / (4.0 * N)
    lower1 = jnp.linalg.cholesky(gram1 + shift * jnp.eye(N, dtype=jnp.float32))
    basis1 = lax.linalg.triangular_solve(lower1, matrix_a, left_side=False, lower=True, transpose_a=True)
    gram2 = jnp.dot(basis1.T.astype(jnp.float32), basis1.astype(jnp.float32), precision=highest, preferred_element_type=jnp.float32)
    lower2 = jnp.linalg.cholesky(gram2)
    basis = lax.linalg.triangular_solve(lower2, basis1, left_side=False, lower=True, transpose_a=True)
    factor = jnp.dot(lower2.T.astype(jnp.float32), lower1.T.astype(jnp.float32), precision=highest, preferred_element_type=jnp.float32)
    projection = jnp.dot(basis.T.astype(jnp.float32), matrix_b.astype(jnp.float32), precision=highest, preferred_element_type=jnp.float32)
    return (lower1.T, factor, projection)
```

```python
import math

import jax
import jax.numpy as jnp
from jax import lax
from jax.experimental import pallas as pl
from jax.experimental.pallas import tpu as pltpu
from jax.sharding import Mesh, PartitionSpec as P


BLOCK = 128
PANEL = 8
GROUP = 4


def dot(lhs, rhs, lhs_dim=1, rhs_dim=0):
    return lax.dot_general(
        lhs,
        rhs,
        (((lhs_dim,), (rhs_dim,)), ((), ())),
        precision=lax.Precision.HIGHEST,
        preferred_element_type=jnp.float32,
    )


def tile(value, count):
    return value if count == 1 else jnp.concatenate([value] * count, axis=0)


def lane(value, index):
    return jnp.broadcast_to(value[:, index : index + 1], value.shape)


def sublane(value, index):
    return jnp.broadcast_to(value[index : index + 1, :], value.shape)


def factor_block(block):
    panels = BLOCK // PANEL
    rows = lax.broadcasted_iota(jnp.int32, (PANEL, BLOCK), 0)
    lanes = lax.broadcasted_iota(jnp.int32, (PANEL, BLOCK), 1)
    left = [block[p * PANEL : (p + 1) * PANEL, :] for p in range(panels)]
    right = [(lanes == rows + p * PANEL).astype(jnp.float32) for p in range(panels)]
    for p in range(panels):
        base = p * PANEL
        own, aug = left[p], right[p]
        cols = [lane(own, base + k) for k in range(PANEL)]
        scales, owns, augs, entries = [], [], [], []
        upper, inverse = own, aug
        for k in range(PANEL):
            scale = lax.rsqrt(sublane(cols[k], k))
            column = cols[k] * scale
            own_row = sublane(own, k) * scale
            aug_row = sublane(aug, k) * scale
            entry = {m: sublane(column, m) for m in range(k + 1, PANEL)}
            for m in range(k + 1, PANEL):
                cols[m] = cols[m] - column * entry[m]
            own = own - column * own_row
            aug = aug - column * aug_row
            upper = jnp.where(rows == k, own_row, upper)
            inverse = jnp.where(rows == k, aug_row, inverse)
            scales.append(scale)
            owns.append(own_row)
            augs.append(aug_row)
            entries.append(entry)
        left[p] = jnp.where(lanes >= rows + base, upper, 0.0)
        right[p] = inverse
        first = p + 1
        while first < panels:
            count = 1 if first == p + 1 else min(GROUP, panels - first)
            height = count * PANEL
            own = jnp.concatenate(left[first : first + count], axis=0) if count > 1 else left[first]
            aug = jnp.concatenate(right[first : first + count], axis=0) if count > 1 else right[first]
            cols = [lane(own, base + k) for k in range(PANEL)]
            for k in range(PANEL):
                column = cols[k] * tile(scales[k], count)
                for m in range(k + 1, PANEL):
                    cols[m] = cols[m] - column * tile(entries[k][m], count)
                own = own - column * tile(owns[k], count)
                aug = aug - column * tile(augs[k], count)
            for q in range(count):
                left[first + q] = own[q * PANEL : (q + 1) * PANEL]
                right[first + q] = aug[q * PANEL : (q + 1) * PANEL]
            first += count
    return jnp.concatenate(left, axis=0), jnp.concatenate(right, axis=0)


def packed_blocks(width):
    count = width // BLOCK
    return [(i, k) for i in range(count) for k in range(i, count)]


def store_gram(matrix_ref, low_ref, high_ref):
    width = matrix_ref.shape[1]
    count = width // BLOCK
    half = low_ref.shape[0] // BLOCK
    place = 0
    for i in range(count):
        product = dot(
            matrix_ref[:, i * BLOCK : (i + 1) * BLOCK], matrix_ref[:, i * BLOCK :], 0, 0
        )
        for k in range(count - i):
            out_ref, at = (low_ref, place) if place < half else (high_ref, place - half)
            out_ref[at * BLOCK : (at + 1) * BLOCK, :] = product[:, k * BLOCK : (k + 1) * BLOCK]
            place += 1


def load_packed(low_ref, high_ref, upper_ref):
    half = low_ref.shape[0] // BLOCK
    for place, (i, k) in enumerate(packed_blocks(upper_ref.shape[1])):
        in_ref, at = (low_ref, place) if place < half else (high_ref, place - half)
        upper_ref[i * BLOCK : (i + 1) * BLOCK, k * BLOCK : (k + 1) * BLOCK] = in_ref[
            at * BLOCK : (at + 1) * BLOCK, :
        ]


def copy_halves(low_ref, high_ref, low_out, high_out):
    low_out[...] = low_ref[...]
    high_out[...] = high_ref[...]


def by_core(core, run, mine_ref, other_ref):
    pl.when(core == 0)(lambda: run(mine_ref, other_ref))
    pl.when(core != 0)(lambda: run(other_ref, mine_ref))


def clear_lower(upper_ref):
    count = upper_ref.shape[1] // BLOCK
    for i in range(1, count):
        upper_ref[i * BLOCK : (i + 1) * BLOCK, : i * BLOCK] = jnp.zeros(
            (BLOCK, i * BLOCK), jnp.float32
        )


def add_shift(upper_ref):
    width = upper_ref.shape[1]
    count = width // BLOCK
    on_diagonal = lax.broadcasted_iota(jnp.int32, (BLOCK, BLOCK), 0) == lax.broadcasted_iota(
        jnp.int32, (BLOCK, BLOCK), 1
    )
    parts = [slice(i * BLOCK, (i + 1) * BLOCK) for i in range(count)]
    total = jnp.zeros((BLOCK, BLOCK), jnp.float32)
    for part in parts:
        total = total + jnp.where(on_diagonal, upper_ref[part, part], 0.0)
    shift = jnp.sum(jnp.sum(total, axis=0, keepdims=True), axis=1, keepdims=True) / (4.0 * width)
    for part in parts:
        block = upper_ref[part, part]
        upper_ref[part, part] = jnp.where(on_diagonal, block + shift, block)


def factorize(upper_ref, inverse_ref, ride_ref=None):
    width = upper_ref.shape[1]
    count = width // BLOCK
    lanes = lax.broadcasted_iota(jnp.int32, (BLOCK, width), 1)

    def step(j, carry):
        begin = pl.multiple_of(j * BLOCK, BLOCK)
        at = pl.ds(begin, BLOCK)
        upper, inverse = factor_block(upper_ref[at, at])
        inverse_ref[at, :] = inverse
        row = jnp.where(lanes >= begin + BLOCK, dot(inverse, upper_ref[at, :]), 0.0)
        upper_ref[at, :] = row
        upper_ref[at, at] = upper
        if ride_ref is not None:
            solved = dot(ride_ref[:, at], inverse, 1, 1)
            ride_ref[...] = ride_ref[...] - dot(solved, row)
            ride_ref[:, at] = solved

        def trail(i, inner):
            below = pl.ds(pl.multiple_of(i * BLOCK, BLOCK), BLOCK)
            upper_ref[below, :] = upper_ref[below, :] - dot(
                upper_ref[at, below], upper_ref[at, :], 0, 0
            )
            return inner

        lax.fori_loop(j + 1, count, trail, 0)
        return carry

    lax.fori_loop(0, count, step, 0)


def solve_rows(rows_ref, upper_ref, inverse_ref, out_ref):
    count = upper_ref.shape[1] // BLOCK
    out_ref[...] = jnp.zeros(out_ref.shape, jnp.float32)
    for j in reversed(range(count)):
        at = slice(j * BLOCK, (j + 1) * BLOCK)
        rest = rows_ref[:, at]
        if j + 1 < count:
            after = slice((j + 1) * BLOCK, count * BLOCK)
            rest = rest - dot(out_ref[:, after], upper_ref[at, after], 1, 1)
        out_ref[:, at] = dot(rest, inverse_ref[at, :])


def gram_kernel(core_ref, matrix_ref, mine_ref, other_ref, low_ref, high_ref):
    store_gram(matrix_ref, low_ref, high_ref)
    by_core(
        core_ref[0], lambda low, high: copy_halves(low_ref, high_ref, low, high), mine_ref, other_ref
    )


def first_kernel(
    core_ref, mine_ref, other_ref, matrix_ref, upper_ref, inverse_ref, mine2_ref, other2_ref,
    ride_ref, low_ref, high_ref,
):
    core = core_ref[0]
    by_core(core, lambda low, high: load_packed(low, high, upper_ref), mine_ref, other_ref)
    clear_lower(upper_ref)
    add_shift(upper_ref)
    ride_ref[...] = matrix_ref[...]
    factorize(upper_ref, inverse_ref, ride_ref)
    store_gram(ride_ref, low_ref, high_ref)
    by_core(core, lambda low, high: copy_halves(low_ref, high_ref, low, high), mine2_ref, other2_ref)


def second_kernel(
    core_ref, start_ref, mine_ref, other_ref, upper1_ref, inverse1_ref, cross_ref,
    first_ref, factor_ref, projection_ref,
    upper_ref, inverse_ref, unit_ref, half_ref, full_ref,
):
    by_core(core_ref[0], lambda low, high: load_packed(low, high, upper_ref), mine_ref, other_ref)
    clear_lower(upper_ref)
    factorize(upper_ref, inverse_ref)
    out_rows, width = first_ref.shape
    start = pl.multiple_of(start_ref[0], out_rows)
    mine = pl.ds(start, out_rows)
    first_ref[...] = upper1_ref[mine, :]
    factor_ref[...] = dot(upper_ref[mine, :], upper1_ref[...])
    lanes = lax.broadcasted_iota(jnp.int32, (out_rows, width), 1)
    rows = lax.broadcasted_iota(jnp.int32, (out_rows, width), 0)
    unit_ref[...] = (lanes == rows + start).astype(jnp.float32)
    solve_rows(unit_ref, upper_ref, inverse_ref, half_ref)
    solve_rows(half_ref, upper1_ref, inverse1_ref, full_ref)
    projection_ref[...] = dot(full_ref[...], cross_ref[...])


VMEM = pl.BlockSpec(memory_space=pltpu.VMEM)
SMEM = pl.BlockSpec(memory_space=pltpu.SMEM)


def floats(*shape):
    return jax.ShapeDtypeStruct(shape, jnp.float32)


def scratch(*shape):
    return pltpu.VMEM(shape, jnp.float32)


def halves(width):
    rows = len(packed_blocks(width)) * BLOCK // 2
    return (floats(rows, BLOCK), floats(rows, BLOCK))


def scratch_halves(width):
    return [scratch(*half.shape) for half in halves(width)]


def gram(core, matrix):
    return pl.pallas_call(
        gram_kernel,
        out_shape=halves(matrix.shape[1]),
        in_specs=[SMEM, VMEM],
        out_specs=(VMEM, VMEM),
        scratch_shapes=scratch_halves(matrix.shape[1]),
    )(core, matrix)


def first_pass(core, mine, other, matrix):
    width = matrix.shape[1]
    return pl.pallas_call(
        first_kernel,
        out_shape=(floats(width, width), floats(width, BLOCK)) + halves(width),
        in_specs=[SMEM, VMEM, VMEM, VMEM],
        out_specs=(VMEM,) * 4,
        scratch_shapes=[scratch(*matrix.shape)] + scratch_halves(width),
    )(core, mine, other, matrix)


def second_pass(core, start, mine, other, upper1, inverse1, cross, out_rows):
    width = upper1.shape[1]
    return pl.pallas_call(
        second_kernel,
        out_shape=(floats(out_rows, width),) * 3,
        in_specs=[SMEM, SMEM, VMEM, VMEM, VMEM, VMEM, VMEM],
        out_specs=(VMEM, VMEM, VMEM),
        scratch_shapes=[
            scratch(width, width),
            scratch(width, BLOCK),
            scratch(out_rows, width),
            scratch(out_rows, width),
            scratch(out_rows, width),
        ],
    )(core, start, mine, other, upper1, inverse1, cross)


def sum_halves(mine, other, beside=None):
    chips = lax.axis_size("chip")
    swap = [(0, 1), (1, 0)]
    part = mine + lax.ppermute(other, "core", swap)
    pieces = lax.all_to_all(part.reshape(chips, -1, BLOCK), "chip", 0, 0, tiled=True)
    piece = jnp.sum(pieces, axis=0, keepdims=True)
    if beside is not None:
        piece, beside = lax.optimization_barrier((piece, beside))
    whole = lax.all_to_all(
        jnp.broadcast_to(piece, pieces.shape), "chip", 0, 0, tiled=True
    ).reshape(part.shape)
    other = lax.ppermute(whole, "core", swap)
    whole, other = in_vmem(whole), in_vmem(other)
    return (whole, other) if beside is None else (whole, other, beside)


def in_vmem(value):
    return pltpu.with_memory_space_constraint(value, pltpu.VMEM)


def per_device(matrix_a, matrix_b):
    width = matrix_a.shape[1]
    axes = ("chip", "core")
    out_rows = width // lax.axis_size(axes)
    start = (lax.axis_index(axes) * out_rows).astype(jnp.int32).reshape(1)
    core = lax.axis_index("core").astype(jnp.int32).reshape(1)
    gram1 = gram(core, matrix_a)
    cross = dot(matrix_a, matrix_b, 0, 0)
    *gram1, cross = lax.optimization_barrier((*gram1, cross))
    cross = lax.psum(cross, axes)
    upper1, inverse1, *gram2 = first_pass(core, *sum_halves(*gram1), matrix_a)
    mine, other, cross = sum_halves(*gram2, cross)
    return second_pass(core, start, mine, other, upper1, inverse1, cross, out_rows)


def solution(mesh):
    groups = mesh.shape["groups"]
    split = Mesh(mesh.devices.reshape(groups, -1, 2), ("groups", "chip", "core"))
    placed = P(("groups", "chip", "core"), None)
    return jax.shard_map(
        per_device,
        mesh=split,
        in_specs=(placed, placed),
        out_specs=(placed, placed, placed),
        check_vma=False,
    )
```

```python
from functools import partial

import jax
import jax.numpy as jnp
from jax import lax
from jax.experimental import pallas as pl
from jax.experimental.pallas import tpu as pltpu
from jax.sharding import Mesh, PartitionSpec as P


BLOCK = 128
PANEL = 8
GROUP = 4


def dot(lhs, rhs, lhs_dim=1, rhs_dim=0):
    return lax.dot_general(
        lhs,
        rhs,
        (((lhs_dim,), (rhs_dim,)), ((), ())),
        precision=lax.Precision.HIGHEST,
        preferred_element_type=jnp.float32,
    )


def tile(value, count):
    return value if count == 1 else jnp.concatenate([value] * count, axis=0)


def lane(value, index):
    return jnp.broadcast_to(value[:, index : index + 1], value.shape)


def sublane(value, index):
    return jnp.broadcast_to(value[index : index + 1, :], value.shape)


def factor_block(block):
    panels = BLOCK // PANEL
    rows = lax.broadcasted_iota(jnp.int32, (PANEL, BLOCK), 0)
    lanes = lax.broadcasted_iota(jnp.int32, (PANEL, BLOCK), 1)
    left = [block[p * PANEL : (p + 1) * PANEL, :] for p in range(panels)]
    right = [(lanes == rows + p * PANEL).astype(jnp.float32) for p in range(panels)]
    for p in range(panels):
        base = p * PANEL
        own, aug = left[p], right[p]
        cols = [lane(own, base + k) for k in range(PANEL)]
        scales, owns, augs, entries = [], [], [], []
        upper, inverse = own, aug
        for k in range(PANEL):
            scale = lax.rsqrt(sublane(cols[k], k))
            column = cols[k] * scale
            own_row = sublane(own, k) * scale
            aug_row = sublane(aug, k) * scale
            entry = {m: sublane(column, m) for m in range(k + 1, PANEL)}
            for m in range(k + 1, PANEL):
                cols[m] = cols[m] - column * entry[m]
            own = own - column * own_row
            aug = aug - column * aug_row
            upper = jnp.where(rows == k, own_row, upper)
            inverse = jnp.where(rows == k, aug_row, inverse)
            scales.append(scale)
            owns.append(own_row)
            augs.append(aug_row)
            entries.append(entry)
        left[p] = jnp.where(lanes >= rows + base, upper, 0.0)
        right[p] = inverse
        first = p + 1
        while first < panels:
            count = 1 if first == p + 1 else min(GROUP, panels - first)
            height = count * PANEL
            own = jnp.concatenate(left[first : first + count], axis=0) if count > 1 else left[first]
            aug = jnp.concatenate(right[first : first + count], axis=0) if count > 1 else right[first]
            cols = [lane(own, base + k) for k in range(PANEL)]
            for k in range(PANEL):
                column = cols[k] * tile(scales[k], count)
                for m in range(k + 1, PANEL):
                    cols[m] = cols[m] - column * tile(entries[k][m], count)
                own = own - column * tile(owns[k], count)
                aug = aug - column * tile(augs[k], count)
            for q in range(count):
                left[first + q] = own[q * PANEL : (q + 1) * PANEL]
                right[first + q] = aug[q * PANEL : (q + 1) * PANEL]
            first += count
    return jnp.concatenate(left, axis=0), jnp.concatenate(right, axis=0)


def packed_blocks(width):
    count = width // BLOCK
    return [(i, k) for i in range(count) for k in range(i, count)]


def store_gram(matrix_ref, low_ref, high_ref):
    width = matrix_ref.shape[1]
    count = width // BLOCK
    half = low_ref.shape[0] // BLOCK
    place = 0
    for i in range(count):
        product = dot(
            matrix_ref[:, i * BLOCK : (i + 1) * BLOCK], matrix_ref[:, i * BLOCK :], 0, 0
        )
        for k in range(count - i):
            out_ref, at = (low_ref, place) if place < half else (high_ref, place - half)
            out_ref[at * BLOCK : (at + 1) * BLOCK, :] = product[:, k * BLOCK : (k + 1) * BLOCK]
            place += 1


def load_packed(low_ref, high_ref, upper_ref):
    half = low_ref.shape[0] // BLOCK
    for place, (i, k) in enumerate(packed_blocks(upper_ref.shape[1])):
        in_ref, at = (low_ref, place) if place < half else (high_ref, place - half)
        upper_ref[i * BLOCK : (i + 1) * BLOCK, k * BLOCK : (k + 1) * BLOCK] = in_ref[
            at * BLOCK : (at + 1) * BLOCK, :
        ]


def copy_halves(low_ref, high_ref, low_out, high_out):
    low_out[...] = low_ref[...]
    high_out[...] = high_ref[...]


def by_core(core, run, mine_ref, other_ref):
    pl.when(core == 0)(lambda: run(mine_ref, other_ref))
    pl.when(core != 0)(lambda: run(other_ref, mine_ref))


def clear_lower(upper_ref):
    count = upper_ref.shape[1] // BLOCK
    for i in range(1, count):
        upper_ref[i * BLOCK : (i + 1) * BLOCK, : i * BLOCK] = jnp.zeros(
            (BLOCK, i * BLOCK), jnp.float32
        )


def add_shift(upper_ref):
    width = upper_ref.shape[1]
    count = width // BLOCK
    on_diagonal = lax.broadcasted_iota(jnp.int32, (BLOCK, BLOCK), 0) == lax.broadcasted_iota(
        jnp.int32, (BLOCK, BLOCK), 1
    )
    parts = [slice(i * BLOCK, (i + 1) * BLOCK) for i in range(count)]
    total = jnp.zeros((BLOCK, BLOCK), jnp.float32)
    for part in parts:
        total = total + jnp.where(on_diagonal, upper_ref[part, part], 0.0)
    shift = jnp.sum(jnp.sum(total, axis=0, keepdims=True), axis=1, keepdims=True) / (4.0 * width)
    for part in parts:
        block = upper_ref[part, part]
        upper_ref[part, part] = jnp.where(on_diagonal, block + shift, block)


def factorize(upper_ref, inverse_ref, turned_ref, ride_ref=None):
    width = upper_ref.shape[1]
    count = width // BLOCK

    def step(j, carry):
        at = pl.ds(pl.multiple_of(j * BLOCK, BLOCK), BLOCK)
        upper, inverse = factor_block(upper_ref[at, at])
        inverse_ref[at, :] = inverse
        upper_ref[at, at] = upper
        for own in range(count):
            pl.when(j == own)(partial(update, own))
        return carry

    def update(j):
        at = slice(j * BLOCK, (j + 1) * BLOCK)
        after = slice((j + 1) * BLOCK, width)
        inverse = inverse_ref[at, :]
        if ride_ref is not None:
            solved = dot(ride_ref[:, at], inverse, 1, 1)
            ride_ref[:, at] = solved
        if j + 1 == count:
            return
        row = dot(inverse, upper_ref[at, after])
        upper_ref[at, after] = row
        turned_ref[after, :] = row.T
        if ride_ref is not None:
            ride_ref[:, after] = ride_ref[:, after] - dot(solved, row)
        begin = j + 1
        while begin < count:
            end = min(count, begin + 2 - begin % 2)
            rows = slice((j + 1) * BLOCK, end * BLOCK)
            columns = slice(begin * BLOCK, end * BLOCK)
            upper_ref[rows, columns] = upper_ref[rows, columns] - dot(
                turned_ref[rows, :], upper_ref[at, columns]
            )
            begin = end

    lax.fori_loop(0, count, step, 0)
    clear_lower(upper_ref)


def solve_rows(rows_ref, upper_ref, inverse_ref, out_ref):
    count = upper_ref.shape[1] // BLOCK
    out_ref[...] = jnp.zeros(out_ref.shape, jnp.float32)
    for j in reversed(range(count)):
        at = slice(j * BLOCK, (j + 1) * BLOCK)
        rest = rows_ref[:, at]
        if j + 1 < count:
            after = slice((j + 1) * BLOCK, count * BLOCK)
            rest = rest - dot(out_ref[:, after], upper_ref[at, after], 1, 1)
        out_ref[:, at] = dot(rest, inverse_ref[at, :])


def gram_kernel(core_ref, matrix_ref, mine_ref, other_ref, low_ref, high_ref):
    store_gram(matrix_ref, low_ref, high_ref)
    by_core(
        core_ref[0], lambda low, high: copy_halves(low_ref, high_ref, low, high), mine_ref, other_ref
    )


def first_kernel(
    core_ref, mine_ref, other_ref, matrix_ref, upper_ref, inverse_ref, mine2_ref, other2_ref,
    ride_ref, turned_ref, low_ref, high_ref,
):
    core = core_ref[0]
    by_core(core, lambda low, high: load_packed(low, high, upper_ref), mine_ref, other_ref)
    add_shift(upper_ref)
    ride_ref[...] = matrix_ref[...]
    factorize(upper_ref, inverse_ref, turned_ref, ride_ref)
    store_gram(ride_ref, low_ref, high_ref)
    by_core(core, lambda low, high: copy_halves(low_ref, high_ref, low, high), mine2_ref, other2_ref)


def second_kernel(
    core_ref, start_ref, mine_ref, other_ref, upper1_ref, inverse1_ref,
    first_ref, factor_ref, solved_ref,
    upper_ref, inverse_ref, turned_ref, unit_ref, half_ref,
):
    by_core(core_ref[0], lambda low, high: load_packed(low, high, upper_ref), mine_ref, other_ref)
    factorize(upper_ref, inverse_ref, turned_ref)
    out_rows, width = first_ref.shape
    start = pl.multiple_of(start_ref[0], out_rows)
    mine = pl.ds(start, out_rows)
    first_ref[...] = upper1_ref[mine, :]
    factor_ref[...] = dot(upper_ref[mine, :], upper1_ref[...])
    lanes = lax.broadcasted_iota(jnp.int32, (out_rows, width), 1)
    rows = lax.broadcasted_iota(jnp.int32, (out_rows, width), 0)
    unit_ref[...] = (lanes == rows + start).astype(jnp.float32)
    solve_rows(unit_ref, upper_ref, inverse_ref, half_ref)
    solve_rows(half_ref, upper1_ref, inverse1_ref, solved_ref)


VMEM = pl.BlockSpec(memory_space=pltpu.VMEM)
SMEM = pl.BlockSpec(memory_space=pltpu.SMEM)


def floats(*shape):
    return jax.ShapeDtypeStruct(shape, jnp.float32)


def scratch(*shape):
    return pltpu.VMEM(shape, jnp.float32)


def halves(width):
    rows = len(packed_blocks(width)) * BLOCK // 2
    return (floats(rows, BLOCK), floats(rows, BLOCK))


def scratch_halves(width):
    return [scratch(*half.shape) for half in halves(width)]


def gram(core, matrix):
    return pl.pallas_call(
        gram_kernel,
        out_shape=halves(matrix.shape[1]),
        in_specs=[SMEM, VMEM],
        out_specs=(VMEM, VMEM),
        scratch_shapes=scratch_halves(matrix.shape[1]),
    )(core, matrix)


def first_pass(core, mine, other, matrix):
    width = matrix.shape[1]
    return pl.pallas_call(
        first_kernel,
        out_shape=(floats(width, width), floats(width, BLOCK)) + halves(width),
        in_specs=[SMEM, VMEM, VMEM, VMEM],
        out_specs=(VMEM,) * 4,
        scratch_shapes=[scratch(*matrix.shape), scratch(width, BLOCK)] + scratch_halves(width),
    )(core, mine, other, matrix)


def second_pass(core, start, mine, other, upper1, inverse1, out_rows):
    width = upper1.shape[1]
    return pl.pallas_call(
        second_kernel,
        out_shape=(floats(out_rows, width),) * 3,
        in_specs=[SMEM, SMEM, VMEM, VMEM, VMEM, VMEM],
        out_specs=(VMEM, VMEM, VMEM),
        scratch_shapes=[
            scratch(width, width),
            scratch(width, BLOCK),
            scratch(width, BLOCK),
            scratch(out_rows, width),
            scratch(out_rows, width),
        ],
    )(core, start, mine, other, upper1, inverse1)


def sum_halves(mine, other):
    chips = lax.axis_size("chip")
    swap = [(0, 1), (1, 0)]
    part = mine + lax.ppermute(other, "core", swap)
    pieces = lax.all_to_all(part.reshape(chips, -1, BLOCK), "chip", 0, 0, tiled=True)
    piece = jnp.sum(pieces, axis=0, keepdims=True)
    whole = lax.all_to_all(
        jnp.broadcast_to(piece, pieces.shape), "chip", 0, 0, tiled=True
    ).reshape(part.shape)
    other = lax.ppermute(whole, "core", swap)
    return in_vmem(whole), in_vmem(other)


def in_vmem(value):
    return pltpu.with_memory_space_constraint(value, pltpu.VMEM)


def per_device(matrix_a, matrix_b):
    width = matrix_a.shape[1]
    axes = ("chip", "core")
    out_rows = width // lax.axis_size(axes)
    start = (lax.axis_index(axes) * out_rows).astype(jnp.int32).reshape(1)
    core = lax.axis_index("core").astype(jnp.int32).reshape(1)
    gram1 = gram(core, matrix_a)
    cross = dot(matrix_a, matrix_b, 0, 0)
    *gram1, cross = lax.optimization_barrier((*gram1, cross))
    cross = lax.psum(cross, axes)
    upper1, inverse1, *gram2 = first_pass(core, *sum_halves(*gram1), matrix_a)
    first, factor, solved = second_pass(
        core, start, *sum_halves(*gram2), upper1, inverse1, out_rows
    )
    solved, cross = lax.optimization_barrier((solved, cross))
    return first, factor, dot(solved, cross)


def solution(mesh):
    groups = mesh.shape["groups"]
    split = Mesh(mesh.devices.reshape(groups, -1, 2), ("groups", "chip", "core"))
    placed = P(("groups", "chip", "core"), None)
    return jax.shard_map(
        per_device,
        mesh=split,
        in_specs=(placed, placed),
        out_specs=(placed, placed, placed),
        check_vma=False,
    )
```

```python
from functools import partial

import jax
import jax.numpy as jnp
from jax import lax
from jax.experimental import pallas as pl
from jax.experimental.pallas import tpu as pltpu
from jax.sharding import Mesh, PartitionSpec as P


BLOCK = 128
PANEL = 8
GROUP = 4


def dot(lhs, rhs, lhs_dim=1, rhs_dim=0):
    return lax.dot_general(
        lhs,
        rhs,
        (((lhs_dim,), (rhs_dim,)), ((), ())),
        precision=lax.Precision.HIGHEST,
        preferred_element_type=jnp.float32,
    )


def tile(value, count):
    return value if count == 1 else jnp.concatenate([value] * count, axis=0)


def lane(value, index):
    return jnp.broadcast_to(value[:, index : index + 1], value.shape)


def sublane(value, index):
    return jnp.broadcast_to(value[index : index + 1, :], value.shape)


def factor_block(block):
    panels = BLOCK // PANEL
    rows = lax.broadcasted_iota(jnp.int32, (PANEL, BLOCK), 0)
    lanes = lax.broadcasted_iota(jnp.int32, (PANEL, BLOCK), 1)
    left = [block[p * PANEL : (p + 1) * PANEL, :] for p in range(panels)]
    right = [(lanes == rows + p * PANEL).astype(jnp.float32) for p in range(panels)]
    ready = [lane(left[0], k) for k in range(PANEL)]
    for p in range(panels):
        base = p * PANEL
        own, aug = left[p], right[p]
        cols = ready
        scales, owns, augs, entries = [], [], [], []
        upper, inverse = own, aug
        for k in range(PANEL):
            scale = lax.rsqrt(sublane(cols[k], k))
            column = cols[k] * scale
            own_row = sublane(own, k) * scale
            aug_row = sublane(aug, k) * scale
            entry = {m: sublane(column, m) for m in range(k + 1, PANEL)}
            for m in range(k + 1, PANEL):
                cols[m] = cols[m] - column * entry[m]
            own = own - column * own_row
            aug = aug - column * aug_row
            upper = jnp.where(rows == k, own_row, upper)
            inverse = jnp.where(rows == k, aug_row, inverse)
            scales.append(scale)
            owns.append(own_row)
            augs.append(aug_row)
            entries.append(entry)
        left[p] = jnp.where(lanes >= rows + base, upper, 0.0)
        right[p] = inverse
        first = p + 1
        while first < panels:
            follows = first == p + 1
            count = 1 if follows else min(GROUP, panels - first)
            height = count * PANEL
            own = jnp.concatenate(left[first : first + count], axis=0) if count > 1 else left[first]
            aug = jnp.concatenate(right[first : first + count], axis=0) if count > 1 else right[first]
            cols = [lane(own, base + k) for k in range(PANEL)]
            if follows:
                ready = [lane(own, base + PANEL + k) for k in range(PANEL)]
            for k in range(PANEL):
                column = cols[k] * tile(scales[k], count)
                if follows:
                    ready = [ready[m] - column * sublane(column, m) for m in range(PANEL)]
                for m in range(k + 1, PANEL):
                    cols[m] = cols[m] - column * tile(entries[k][m], count)
                own = own - column * tile(owns[k], count)
                aug = aug - column * tile(augs[k], count)
            for q in range(count):
                left[first + q] = own[q * PANEL : (q + 1) * PANEL]
                right[first + q] = aug[q * PANEL : (q + 1) * PANEL]
            first += count
    return jnp.concatenate(left, axis=0), jnp.concatenate(right, axis=0)


def packed_blocks(width):
    count = width // BLOCK
    return [(i, k) for i in range(count) for k in range(i, count)]


def store_gram(matrix_ref, low_ref, high_ref):
    width = matrix_ref.shape[1]
    count = width // BLOCK
    half = low_ref.shape[0] // BLOCK
    place = 0
    for i in range(count):
        product = dot(
            matrix_ref[:, i * BLOCK : (i + 1) * BLOCK], matrix_ref[:, i * BLOCK :], 0, 0
        )
        for k in range(count - i):
            out_ref, at = (low_ref, place) if place < half else (high_ref, place - half)
            out_ref[at * BLOCK : (at + 1) * BLOCK, :] = product[:, k * BLOCK : (k + 1) * BLOCK]
            place += 1


def load_packed(low_ref, high_ref, upper_ref):
    half = low_ref.shape[0] // BLOCK
    for place, (i, k) in enumerate(packed_blocks(upper_ref.shape[1])):
        in_ref, at = (low_ref, place) if place < half else (high_ref, place - half)
        upper_ref[i * BLOCK : (i + 1) * BLOCK, k * BLOCK : (k + 1) * BLOCK] = in_ref[
            at * BLOCK : (at + 1) * BLOCK, :
        ]


def copy_halves(low_ref, high_ref, low_out, high_out):
    low_out[...] = low_ref[...]
    high_out[...] = high_ref[...]


def by_core(core, run, mine_ref, other_ref):
    pl.when(core == 0)(lambda: run(mine_ref, other_ref))
    pl.when(core != 0)(lambda: run(other_ref, mine_ref))


def clear_lower(upper_ref):
    count = upper_ref.shape[1] // BLOCK
    for i in range(1, count):
        upper_ref[i * BLOCK : (i + 1) * BLOCK, : i * BLOCK] = jnp.zeros(
            (BLOCK, i * BLOCK), jnp.float32
        )


def add_shift(upper_ref):
    width = upper_ref.shape[1]
    count = width // BLOCK
    on_diagonal = lax.broadcasted_iota(jnp.int32, (BLOCK, BLOCK), 0) == lax.broadcasted_iota(
        jnp.int32, (BLOCK, BLOCK), 1
    )
    parts = [slice(i * BLOCK, (i + 1) * BLOCK) for i in range(count)]
    total = jnp.zeros((BLOCK, BLOCK), jnp.float32)
    for part in parts:
        total = total + jnp.where(on_diagonal, upper_ref[part, part], 0.0)
    shift = jnp.sum(jnp.sum(total, axis=0, keepdims=True), axis=1, keepdims=True) / (4.0 * width)
    for part in parts:
        block = upper_ref[part, part]
        upper_ref[part, part] = jnp.where(on_diagonal, block + shift, block)


def factorize(upper_ref, inverse_ref, turned_ref, ride_ref=None):
    width = upper_ref.shape[1]
    count = width // BLOCK

    def step(j, carry):
        at = pl.ds(pl.multiple_of(j * BLOCK, BLOCK), BLOCK)
        upper, inverse = factor_block(upper_ref[at, at])
        inverse_ref[at, :] = inverse
        upper_ref[at, at] = upper
        for own in range(count):
            pl.when(j == own)(partial(update, own))
        return carry

    def update(j):
        at = slice(j * BLOCK, (j + 1) * BLOCK)
        after = slice((j + 1) * BLOCK, width)
        inverse = inverse_ref[at, :]
        if ride_ref is not None:
            solved = dot(ride_ref[:, at], inverse, 1, 1)
            ride_ref[:, at] = solved
        if j + 1 == count:
            return
        row = dot(inverse, upper_ref[at, after])
        upper_ref[at, after] = row
        turned_ref[after, :] = row.T
        if ride_ref is not None:
            ride_ref[:, after] = ride_ref[:, after] - dot(solved, row)
        begin = j + 1
        while begin < count:
            end = min(count, begin + 2 - begin % 2)
            rows = slice((j + 1) * BLOCK, end * BLOCK)
            columns = slice(begin * BLOCK, end * BLOCK)
            upper_ref[rows, columns] = upper_ref[rows, columns] - dot(
                turned_ref[rows, :], upper_ref[at, columns]
            )
            begin = end

    lax.fori_loop(0, count, step, 0)
    clear_lower(upper_ref)


def solve_rows(rows_ref, upper_ref, inverse_ref, out_ref):
    count = upper_ref.shape[1] // BLOCK
    out_ref[...] = jnp.zeros(out_ref.shape, jnp.float32)
    for j in reversed(range(count)):
        at = slice(j * BLOCK, (j + 1) * BLOCK)
        rest = rows_ref[:, at]
        if j + 1 < count:
            after = slice((j + 1) * BLOCK, count * BLOCK)
            rest = rest - dot(out_ref[:, after], upper_ref[at, after], 1, 1)
        out_ref[:, at] = dot(rest, inverse_ref[at, :])


def gram_kernel(core_ref, matrix_ref, mine_ref, other_ref, low_ref, high_ref):
    store_gram(matrix_ref, low_ref, high_ref)
    by_core(
        core_ref[0], lambda low, high: copy_halves(low_ref, high_ref, low, high), mine_ref, other_ref
    )


def first_kernel(
    core_ref, mine_ref, other_ref, matrix_ref, upper_ref, inverse_ref, mine2_ref, other2_ref,
    ride_ref, turned_ref, low_ref, high_ref,
):
    core = core_ref[0]
    by_core(core, lambda low, high: load_packed(low, high, upper_ref), mine_ref, other_ref)
    add_shift(upper_ref)
    ride_ref[...] = matrix_ref[...]
    factorize(upper_ref, inverse_ref, turned_ref, ride_ref)
    store_gram(ride_ref, low_ref, high_ref)
    by_core(core, lambda low, high: copy_halves(low_ref, high_ref, low, high), mine2_ref, other2_ref)


def second_kernel(
    core_ref, start_ref, mine_ref, other_ref, upper1_ref, inverse1_ref,
    first_ref, factor_ref, solved_ref,
    upper_ref, inverse_ref, turned_ref, unit_ref, half_ref,
):
    by_core(core_ref[0], lambda low, high: load_packed(low, high, upper_ref), mine_ref, other_ref)
    factorize(upper_ref, inverse_ref, turned_ref)
    out_rows, width = first_ref.shape
    start = pl.multiple_of(start_ref[0], out_rows)
    mine = pl.ds(start, out_rows)
    first_ref[...] = upper1_ref[mine, :]
    factor_ref[...] = dot(upper_ref[mine, :], upper1_ref[...])
    lanes = lax.broadcasted_iota(jnp.int32, (out_rows, width), 1)
    rows = lax.broadcasted_iota(jnp.int32, (out_rows, width), 0)
    unit_ref[...] = (lanes == rows + start).astype(jnp.float32)
    solve_rows(unit_ref, upper_ref, inverse_ref, half_ref)
    solve_rows(half_ref, upper1_ref, inverse1_ref, solved_ref)


VMEM = pl.BlockSpec(memory_space=pltpu.VMEM)
SMEM = pl.BlockSpec(memory_space=pltpu.SMEM)


def floats(*shape):
    return jax.ShapeDtypeStruct(shape, jnp.float32)


def scratch(*shape):
    return pltpu.VMEM(shape, jnp.float32)


def halves(width):
    rows = len(packed_blocks(width)) * BLOCK // 2
    return (floats(rows, BLOCK), floats(rows, BLOCK))


def scratch_halves(width):
    return [scratch(*half.shape) for half in halves(width)]


def gram(core, matrix):
    return pl.pallas_call(
        gram_kernel,
        out_shape=halves(matrix.shape[1]),
        in_specs=[SMEM, VMEM],
        out_specs=(VMEM, VMEM),
        scratch_shapes=scratch_halves(matrix.shape[1]),
    )(core, matrix)


def first_pass(core, mine, other, matrix):
    width = matrix.shape[1]
    return pl.pallas_call(
        first_kernel,
        out_shape=(floats(width, width), floats(width, BLOCK)) + halves(width),
        in_specs=[SMEM, VMEM, VMEM, VMEM],
        out_specs=(VMEM,) * 4,
        scratch_shapes=[scratch(*matrix.shape), scratch(width, BLOCK)] + scratch_halves(width),
    )(core, mine, other, matrix)


def second_pass(core, start, mine, other, upper1, inverse1, out_rows):
    width = upper1.shape[1]
    return pl.pallas_call(
        second_kernel,
        out_shape=(floats(out_rows, width),) * 3,
        in_specs=[SMEM, SMEM, VMEM, VMEM, VMEM, VMEM],
        out_specs=(VMEM, VMEM, VMEM),
        scratch_shapes=[
            scratch(width, width),
            scratch(width, BLOCK),
            scratch(width, BLOCK),
            scratch(out_rows, width),
            scratch(out_rows, width),
        ],
    )(core, start, mine, other, upper1, inverse1)


def sum_halves(mine, other):
    chips = lax.axis_size("chip")
    swap = [(0, 1), (1, 0)]
    part = mine + lax.ppermute(other, "core", swap)
    pieces = lax.all_to_all(part.reshape(chips, -1, BLOCK), "chip", 0, 0, tiled=True)
    piece = jnp.sum(pieces, axis=0, keepdims=True)
    whole = lax.all_to_all(
        jnp.broadcast_to(piece, pieces.shape), "chip", 0, 0, tiled=True
    ).reshape(part.shape)
    other = lax.ppermute(whole, "core", swap)
    return in_vmem(whole), in_vmem(other)


def in_vmem(value):
    return pltpu.with_memory_space_constraint(value, pltpu.VMEM)


def per_device(matrix_a, matrix_b):
    width = matrix_a.shape[1]
    axes = ("chip", "core")
    out_rows = width // lax.axis_size(axes)
    start = (lax.axis_index(axes) * out_rows).astype(jnp.int32).reshape(1)
    core = lax.axis_index("core").astype(jnp.int32).reshape(1)
    half = width // 2
    swap = [(0, 1), (1, 0)]
    on_first = core[0] == 0
    cross = dot(matrix_a, matrix_b, 0, 0)
    cross, matrix_a = lax.optimization_barrier((cross, matrix_a))
    low, high = cross[:half], cross[half:]
    away = lax.ppermute(jnp.where(on_first, high, low), "core", swap)
    gram1 = gram(core, matrix_a)
    *gram1, away = lax.optimization_barrier((*gram1, away))
    cross = jnp.where(on_first, low, high) + away
    *gram1, cross = lax.optimization_barrier((*gram1, cross))
    cross = lax.psum(cross, "chip")
    upper1, inverse1, *gram2 = first_pass(core, *sum_halves(*gram1), matrix_a)
    first, factor, solved = second_pass(
        core, start, *sum_halves(*gram2), upper1, inverse1, out_rows
    )
    solved, cross = lax.optimization_barrier((solved, cross))
    away = lax.ppermute(cross, "core", swap)
    mine_part = jnp.where(on_first, solved[:, :half], solved[:, half:])
    away_part = jnp.where(on_first, solved[:, half:], solved[:, :half])
    return first, factor, dot(mine_part, cross) + dot(away_part, away)


def solution(mesh):
    groups = mesh.shape["groups"]
    split = Mesh(mesh.devices.reshape(groups, -1, 2), ("groups", "chip", "core"))
    placed = P(("groups", "chip", "core"), None)
    return jax.shard_map(
        per_device,
        mesh=split,
        in_specs=(placed, placed),
        out_specs=(placed, placed, placed),
        check_vma=False,
    )
```
